32 devices in a mesh: gz: 2 (over y), row: 4 (over z), col: 4 (over x, core).
Axes of the slice: x: 2, y: 2, z: 4, core: 2. Of those that a mesh axis runs over, the one named last changes fastest.
Arguments:
- lpanel: bfloat16 [2, 2, 1024, 2048], P(None, 'gz', 'row', 'col'), may hold values from -6 to 6
- upanel: bfloat16 [2, 2, 2048, 4096], P(None, 'gz', 'row', 'col'), may hold values from -0.125 to 0.125
- rowmap: int32 [2, 2, 4], P(None, 'gz', 'row'), may hold values from 0 to 1
- colmap: int32 [2, 2, 16], P(None, 'gz', 'col'), may hold values from 0 to 1
- blockmask: int32 [2, 2, 4, 16], P(None, 'gz', 'row', 'col'), may hold values 0 or 1
- front_blocks: bfloat16 [2, 2048, 2048], P(None, 'row', ('gz', 'col')), may hold values from -6 to 6
Outputs:
- front_update: bfloat16 [2, 2048, 2048], P(None, 'row', ('gz', 'col'))
The draws below stay inside these ranges and needn't reach their ends.
All inputs are finite; a program needn't handle non-finite values. No bound on the sum of `blockmask` on one device may be relied on, other than what follows from the above.
Results may differ from the reference program's by a relative error of at most 0.008.
Values may be sent and summed in bfloat16 or wider, within the bound.
A program may use at most 64 MiB of HBM per device.

```python
import math
import jax
import jax.numpy as jnp
import numpy as np
from jax import lax

B = 256
W = 2048
CB = 4
FRB = 2
LEVELS = 2
UR = 1024
UC = 4096
FR = 2048
FC = 2048
N_GZ = 2
N_ROW = 4
N_COL = 4


def set_ends(values, rng, low, top_value):
    extent = values.shape
    place = [jax.random.randint(jax.random.fold_in(rng, axis), (), 0, extent[axis]) for axis in range(len(extent))]
    values = values.at[tuple(place)].set(low)
    longest = extent.index(max(extent))
    place[longest] = (place[longest] + 1) % extent[longest]
    return values.at[tuple(place)].set(top_value)


def level_of(rng, extent, cuts, least, top_value):
    gain = 1.0
    for position, blocks in cuts:
        draws = jax.random.uniform(jax.random.fold_in(jax.random.fold_in(rng, 6), position), (blocks,), jnp.float32, least / len(cuts), top_value / len(cuts))
        gain = gain * jnp.repeat(jnp.exp(draws), extent[position] // blocks).reshape((-1,) + (1,) * (len(extent) - 1 - position))
    return gain


def rank_bounds(amount, slope):
    portions = [(1 << 20) // math.isqrt(standing ** slope) + 1 for standing in range(1, amount + 1)]
    spread = 1 + sum(portions) // (1 << 30)
    return np.cumsum(np.array([max(1, weight // spread) for weight in portions]))


def ranked(own_key, extent, amount, slope):
    table = rank_bounds(amount, slope)
    pick = jax.random.randint(jax.random.fold_in(own_key, 1), extent, 0, int(table[amount - 1]))
    rank = jnp.searchsorted(jnp.asarray(table, jnp.int32), pick, side="right")
    return jax.random.permutation(jax.random.fold_in(own_key, 2), amount)[rank].astype(jnp.int32)


def gaussian(rng, shape, width, limit, pieces=(), kind=jnp.bfloat16):
    values = jax.random.normal(rng, shape, jnp.float32) * width
    if len(pieces) > 0:
        values = level_of(rng, shape, pieces, -0.22, 0.18) * values
    return jnp.clip(values, min=-limit, max=limit).astype(kind)


def setup_inputs(seed: int = 0) -> dict:
    key_list = jax.random.split(jax.random.key(seed), 7)
    lpanel = gaussian(key_list[0], (LEVELS, N_GZ, UR, W), 1.0, 6.0, ((1, 2), (2, 4), (3, 4)))
    upanel = gaussian(key_list[1], (LEVELS, N_GZ, W, UC), W ** -0.5, 0.125, ((1, 2), (2, 4), (3, 4)))
    rowmap = set_ends(jax.random.randint(key_list[2], (LEVELS, N_GZ, N_ROW), 0, FRB), jax.random.fold_in(key_list[2], 1), 0, FRB - 1).astype(jnp.int32)
    colmap = set_ends(ranked(key_list[3], (LEVELS, N_GZ, N_COL * CB), N_GZ, 2), jax.random.fold_in(key_list[3], 3), 0, N_GZ - 1).astype(jnp.int32)
    blockmask = set_ends((jax.random.randint(key_list[4], (LEVELS, N_GZ, N_ROW, N_COL * CB), 0, 4) < 3).astype(jnp.int32), jax.random.fold_in(key_list[4], 1), 0, 1)
    front_blocks = gaussian(key_list[5], (LEVELS, FR, FC), 1.0, 6.0, ((1, 4), (2, 8)))
    return dict(lpanel=lpanel, upanel=upanel, rowmap=rowmap, colmap=colmap, blockmask=blockmask, front_blocks=front_blocks)


def layer_partial(schur, rows_of, cols_of, live):
    blocks = schur.reshape(N_ROW, B, N_COL, CB, B)
    targets = cols_of.reshape(N_COL, CB)[:, :, None] == jnp.arange(N_GZ, dtype=jnp.int32)[None, None, :]
    col_select = targets.astype(jnp.float32)[None] * live.reshape(N_ROW, N_COL, CB).astype(jnp.float32)[:, :, :, None]
    col_sums = jnp.einsum("rbcjk,rcjl->rblck", blocks, col_select, precision=lax.Precision.HIGHEST)
    row_select = (rows_of[:, None] == jnp.arange(FRB, dtype=jnp.int32)[None, :]).astype(jnp.float32)
    placed = row_select[:, :, None, None, None, None] * col_sums[:, None]
    return placed.reshape(FR, FC)


def reference(lpanel, upanel, rowmap, colmap, blockmask, front_blocks):
    results = []
    for depth in range(LEVELS):
        total = jnp.zeros((FR, FC), jnp.float32)
        for layer in range(N_GZ):
            schur = jnp.dot(lpanel[depth, layer], upanel[depth, layer], preferred_element_type=jnp.float32)
            partial_value = layer_partial(schur, rowmap[depth, layer], colmap[depth, layer], blockmask[depth, layer])
            total = total + partial_value.astype(jnp.bfloat16).astype(jnp.float32)
        results.append((front_blocks[depth].astype(jnp.float32) - total).astype(jnp.bfloat16))
    return jnp.stack(results)
```

```python
import functools

import jax
import jax.numpy as jnp
from jax import lax
from jax.experimental import pallas as pl
from jax.experimental.pallas import tpu as pltpu
from jax.sharding import PartitionSpec as P

CB = 4
FRB = 2
MESH = pl.DeviceIdType.MESH


def column_sums(schur, cols_of, live, layers):
    width = schur.shape[0]
    blocks = schur.reshape(width, CB, width)
    targets = cols_of[:, None] == jnp.arange(layers, dtype=jnp.int32)[None, :]
    col_select = targets.astype(jnp.float32) * live.astype(jnp.float32)[:, None]
    return jnp.einsum("bjk,jl->lbk", blocks, col_select, precision=lax.Precision.HIGHEST)


def general(lpanel, upanel, rowmap, colmap, blockmask, front_blocks):
    layers = lax.axis_size("gz")
    width = lpanel.shape[2]
    levels = lpanel.shape[0]
    tiles = []
    for depth in range(levels):
        left_rows = lax.all_gather(lpanel[depth, 0], "col", axis=1, tiled=True)
        tiles.append(
            jnp.dot(
                left_rows,
                lax.all_gather(upanel[depth, 0], "row", axis=0, tiled=True),
                preferred_element_type=jnp.float32,
            )
        )
    results = []
    every_row = lax.all_gather(rowmap[:, :, 0], "gz", axis=1, tiled=True)
    for depth in range(levels):
        sums = column_sums(tiles[depth], colmap[depth, 0], blockmask[depth, 0, 0], layers).astype(
            jnp.bfloat16
        )
        arrived = lax.all_to_all(sums, "gz", split_axis=0, concat_axis=0, tiled=True)
        row_select = (
            every_row[depth][:, None] == jnp.arange(FRB, dtype=jnp.int32)[None, :]
        ).astype(jnp.float32)
        placed = jnp.einsum(
            "sf,sbk->fbk", row_select, arrived.astype(jnp.float32), precision=lax.Precision.HIGHEST
        )
        placed = placed.reshape(FRB * width, width)
        results.append((front_blocks[depth].astype(jnp.float32) - placed).astype(jnp.bfloat16))
    return jnp.stack(results)


def kernel(
    rows, cols, layers, levels, width,
    l_ref, u_hbm, coef_ref, rm_ref, front_hbm, out_ref,
    u_ref, front_ref, crossed, l_all, coef_all, own, part, p_in, y_out, y_in, rm_in,
    in_sem, x_send, x_recv, l_send, l_recv, loc_sem, relay_send, m_send, m_recv, m_loc,
    p_send, p_recv, y_send, y_recv, rm_send, rm_recv,
):
    z = lax.axis_index("row")
    c = lax.axis_index("col")
    g = lax.axis_index("gz")
    far = lax.rem(c + cols // 2, cols)
    mate = c + 1 - 2 * lax.rem(c, 2)
    other = 1 - g
    gate = lax.rem(c, 2) == lax.rem(z, 2)

    loads = [pltpu.make_async_copy(u_hbm.at[v], u_ref.at[v], in_sem.at[v]) for v in range(levels)]
    loads.append(pltpu.make_async_copy(front_hbm, front_ref, in_sem.at[levels]))
    for load in loads:
        load.start()

    barrier = pltpu.get_barrier_semaphore()
    for step in range(1, rows):
        pl.semaphore_signal(
            barrier, inc=1, device_id={"row": lax.rem(z + step, rows)}, device_id_type=MESH
        )
    pl.semaphore_signal(barrier, inc=1, device_id={"col": far}, device_id_type=MESH)
    pl.semaphore_signal(barrier, inc=1, device_id={"col": mate}, device_id_type=MESH)
    pl.semaphore_signal(barrier, inc=1, device_id={"gz": other}, device_id_type=MESH)
    pl.semaphore_wait(barrier, rows + 2)

    def remote(src, dst, send, recv, where):
        return pltpu.make_async_remote_copy(
            src_ref=src, dst_ref=dst, send_sem=send, recv_sem=recv,
            device_id=where, device_id_type=MESH,
        )

    own_coef = pltpu.make_async_copy(coef_ref, coef_all.at[z], m_loc)
    own_coef.start()
    coef_out = []
    for step in range(1, rows):
        to = lax.rem(z + step, rows)
        coef_out.append(
            remote(coef_ref, coef_all.at[z], m_send.at[step], m_recv.at[z], {"row": to})
        )
        coef_out[-1].start()
    rm_copy = remote(rm_ref, rm_in, rm_send, rm_recv, {"gz": other})
    rm_copy.start()

    across = [
        remote(l_ref.at[v], crossed.at[v], x_send.at[v], x_recv.at[v], {"col": far})
        for v in range(levels)
    ]

    def place(v, half):
        k = c if half == 0 else far
        block = l_ref.at[v] if half == 0 else crossed.at[v]
        copy = remote(block, l_all.at[v, z], l_send.at[v, half], l_recv.at[v, z], {"row": k})
        local = pltpu.make_async_copy(block, l_all.at[v, z], loc_sem.at[v])
        return k, copy, local

    def start_place(v, half):
        k, copy, local = place(v, half)

        @pl.when(k != z)
        def _():
            copy.start()

        @pl.when(k == z)
        def _():
            local.start()

    for v in range(levels):
        across[v].start()
    start_place(0, 0)
    across[0].wait_recv()
    start_place(0, 1)
    for v in range(1, levels):
        start_place(v, 0)
        across[v].wait_recv()
        start_place(v, 1)

    own_coef.wait()
    for step in range(1, rows):
        src = lax.rem(z + step, rows)
        remote(coef_ref, coef_all.at[src], m_send.at[step], m_recv.at[src], {"row": src}).wait_recv()

    def item(v, i):
        odd = lax.rem(i, 2)
        a = (1 - odd) * (rows - 1 - i // 2) + odd * (i // 2)
        relay = remote(
            l_all.at[v, a], l_all.at[v, a], relay_send.at[v, a], l_recv.at[v, a], {"col": mate}
        )

        @pl.when(gate)
        def _():
            @pl.when(a == z)
            def _():
                pltpu.make_async_copy(l_ref.at[v], l_all.at[v, z], loc_sem.at[v]).wait()

            @pl.when(a != z)
            def _():
                relay.wait_recv()

            relay.start()

        @pl.when(jnp.logical_not(gate))
        def _():
            relay.wait_recv()

        left = l_all[v, a]
        for j in range(CB):
            lanes = slice(j * width, (j + 1) * width)
            t = jnp.dot(left, u_ref[v, :, lanes], preferred_element_type=jnp.float32)
            for l in range(layers):
                m = coef_all[a, pl.ds(v * layers + l, 1), lanes]
                if j == 0:
                    own[v, l] = t * m
                else:
                    own[v, l] += t * m

        def send(side, to):
            for l in range(layers):
                part[v, a, l] = own[v, l].astype(jnp.bfloat16)
            remote(
                part.at[v, a], p_in.at[v, side, a], p_send.at[v, a], p_recv.at[v, side, a], {"row": to}
            ).start()

        def forward(side, to, has_up):
            @pl.when(has_up)
            def _():
                remote(
                    part.at[v, a], p_in.at[v, side, a], p_send.at[v, a], p_recv.at[v, side, a], {"row": to}
                ).wait_recv()
                for l in range(layers):
                    own[v, l] += p_in[v, side, a, l].astype(jnp.float32)

            send(side, to)

        @pl.when(a > z)
        def _():
            forward(0, lax.rem(z + 1, rows), z > 0)

        @pl.when(a < z)
        def _():
            forward(1, lax.rem(z + rows - 1, rows), z < rows - 1)

        @pl.when(a == z)
        def _():
            for l in range(layers):
                own[levels + v, l] = own[v, l]

    def run(v):
        def body(i, carry):
            item(v, i)
            return carry

        lax.fori_loop(0, rows, body, 0)

    for v in range(levels):
        loads[v].wait()
        run(v)

    ways = []
    for v in range(levels):
        for side, there in ((0, z > 0), (1, z < rows - 1)):
            @pl.when(there)
            def _(side=side):
                remote(
                    part.at[v, z], p_in.at[v, side, z], p_send.at[v, z], p_recv.at[v, side, z], {"gz": other}
                ).wait_recv()
                for l in range(layers):
                    own[levels + v, l] += p_in[v, side, z, l].astype(jnp.float32)

        y_out[v] = own[levels + v, other].astype(jnp.bfloat16)
        way = remote(y_out.at[v], y_in.at[v], y_send.at[v], y_recv.at[v], {"gz": other})
        way.start()
        ways.append(way)

    loads[levels].wait()
    rm_copy.wait()
    for v in range(levels):
        mine = own[levels + v, g].astype(jnp.bfloat16).astype(jnp.float32)
        ways[v].wait_recv()
        theirs = y_in[v].astype(jnp.float32)
        for f in range(FRB):
            lines = slice(f * width, (f + 1) * width)
            here = (rm_ref[v : v + 1, :] == f).astype(jnp.float32)
            away = (rm_in[v : v + 1, :] == f).astype(jnp.float32)
            total = here * mine + away * theirs
            out_ref[v, lines, :] = (front_ref[v, lines, :].astype(jnp.float32) - total).astype(
                out_ref.dtype
            )

    for copy in coef_out:
        copy.wait_send()
    for v in range(levels):
        across[v].wait_send()
        ways[v].wait_send()
        for half in range(2):
            k, copy, _local = place(v, half)
            pl.when(k != z)(copy.wait_send)
        for a in range(rows):
            relay = remote(
                l_all.at[v, a], l_all.at[v, a], relay_send.at[v, a], l_recv.at[v, a], {"col": mate}
            )
            pl.when(gate)(relay.wait_send)
            sent = remote(
                part.at[v, a], p_in.at[v, 0, a], p_send.at[v, a], p_recv.at[v, 0, a], {"gz": other}
            )
            pl.when(a != z)(sent.wait_send)


def stationary(rows, cols, layers, lpanel, upanel, rowmap, colmap, blockmask, front_blocks):
    levels, _, width, depth = lpanel.shape
    wide = upanel.shape[3]
    select = colmap[:, 0, None, :] == jnp.arange(layers, dtype=jnp.int32)[None, :, None]
    coef = select.astype(jnp.float32) * blockmask[:, 0, 0, None, :].astype(jnp.float32)
    coef = jnp.broadcast_to(coef[..., None], (levels, layers, CB, width))
    coef = coef.reshape(levels * layers, wide)
    rm = jnp.broadcast_to(rowmap[:, 0], (levels, width))
    bf16 = jnp.bfloat16
    vmem = pl.BlockSpec(memory_space=pltpu.VMEM)
    hbm = pl.BlockSpec(memory_space=pl.ANY)
    dma = pltpu.SemaphoreType.DMA
    return pl.pallas_call(
        functools.partial(kernel, rows, cols, layers, levels, width),
        out_shape=jax.ShapeDtypeStruct(front_blocks.shape, front_blocks.dtype),
        in_specs=[vmem, hbm, vmem, vmem, hbm],
        out_specs=vmem,
        scratch_shapes=[
            pltpu.VMEM(upanel[:, 0].shape, bf16),
            pltpu.VMEM(front_blocks.shape, bf16),
            pltpu.VMEM((levels, width, depth), bf16),
            pltpu.VMEM((levels, rows, width, depth), bf16),
            pltpu.VMEM((rows, levels * layers, wide), jnp.float32),
            pltpu.VMEM((2 * levels, layers, width, width), jnp.float32),
            pltpu.VMEM((levels, rows, layers, width, width), bf16),
            pltpu.VMEM((levels, 2, rows, layers, width, width), bf16),
            pltpu.VMEM((levels, width, width), bf16),
            pltpu.VMEM((levels, width, width), bf16),
            pltpu.VMEM((levels, width), jnp.int32),
            dma((levels + 1,)),
            dma((levels,)),
            dma((levels,)),
            dma((levels, 2)),
            dma((levels, rows)),
            dma((levels,)),
            dma((levels, rows)),
            dma((rows,)),
            dma((rows,)),
            dma,
            dma((levels, rows)),
            dma((levels, 2, rows)),
            dma((levels,)),
            dma((levels,)),
            dma,
            dma,
        ],
        compiler_params=pltpu.CompilerParams(collective_id=0, has_side_effects=True),
    )(lpanel[:, 0], upanel[:, 0], coef, rm, front_blocks)


def solution(mesh):
    rows, cols, layers = mesh.shape["row"], mesh.shape["col"], mesh.shape["gz"]
    body = general
    if rows == cols == 2 * layers and layers == 2:
        body = functools.partial(stationary, rows, cols, layers)
    return jax.shard_map(
        body,
        mesh=mesh,
        in_specs=(
            P(None, "gz", "row", "col"),
            P(None, "gz", "row", "col"),
            P(None, "gz", "row"),
            P(None, "gz", "col"),
            P(None, "gz", "row", "col"),
            P(None, "row", ("gz", "col")),
        ),
        out_specs=P(None, "row", ("gz", "col")),
        check_vma=False,
    )
```

```python
import functools

import jax
import jax.numpy as jnp
from jax import lax
from jax.experimental import pallas as pl
from jax.experimental.pallas import tpu as pltpu
from jax.sharding import PartitionSpec as P

CB = 4
FRB = 2
MESH = pl.DeviceIdType.MESH


def column_sums(schur, cols_of, live, layers):
    width = schur.shape[0]
    blocks = schur.reshape(width, CB, width)
    targets = cols_of[:, None] == jnp.arange(layers, dtype=jnp.int32)[None, :]
    col_select = targets.astype(jnp.float32) * live.astype(jnp.float32)[:, None]
    return jnp.einsum("bjk,jl->lbk", blocks, col_select, precision=lax.Precision.HIGHEST)


def general(lpanel, upanel, rowmap, colmap, blockmask, front_blocks):
    layers = lax.axis_size("gz")
    width = lpanel.shape[2]
    levels = lpanel.shape[0]
    tiles = []
    for depth in range(levels):
        left_rows = lax.all_gather(lpanel[depth, 0], "col", axis=1, tiled=True)
        tiles.append(
            jnp.dot(
                left_rows,
                lax.all_gather(upanel[depth, 0], "row", axis=0, tiled=True),
                preferred_element_type=jnp.float32,
            )
        )
    results = []
    every_row = lax.all_gather(rowmap[:, :, 0], "gz", axis=1, tiled=True)
    for depth in range(levels):
        sums = column_sums(tiles[depth], colmap[depth, 0], blockmask[depth, 0, 0], layers).astype(
            jnp.bfloat16
        )
        arrived = lax.all_to_all(sums, "gz", split_axis=0, concat_axis=0, tiled=True)
        row_select = (
            every_row[depth][:, None] == jnp.arange(FRB, dtype=jnp.int32)[None, :]
        ).astype(jnp.float32)
        placed = jnp.einsum(
            "sf,sbk->fbk", row_select, arrived.astype(jnp.float32), precision=lax.Precision.HIGHEST
        )
        placed = placed.reshape(FRB * width, width)
        results.append((front_blocks[depth].astype(jnp.float32) - placed).astype(jnp.bfloat16))
    return jnp.stack(results)


def kernel(
    rows, cols, layers, levels, width,
    l_hbm, u_hbm, cm_ref, live_ref, rm_ref, front_hbm, out_ref,
    l_ref, u_ref, front_ref, crossed, l_all, live_all, own, part, p_in, y_out, y_in, rm_in,
    in_sem, x_send, x_recv, l_send, l_recv, loc_sem, relay_send, m_send, m_recv, m_loc,
    p_send, p_recv, y_send, y_recv, rm_send, rm_recv,
):
    z = lax.axis_index("row")
    c = lax.axis_index("col")
    g = lax.axis_index("gz")
    far = lax.rem(c + cols // 2, cols)
    mate = c + 1 - 2 * lax.rem(c, 2)
    other = 1 - g
    gate = lax.rem(c, 2) == lax.rem(z, 2)

    loads = [pltpu.make_async_copy(u_hbm.at[v], u_ref.at[v], in_sem.at[v]) for v in range(levels)]
    loads.append(pltpu.make_async_copy(front_hbm, front_ref, in_sem.at[levels]))
    first = pltpu.make_async_copy(l_hbm, l_ref, in_sem.at[levels + 1])
    first.start()
    for load in loads:
        load.start()

    barrier = pltpu.get_barrier_semaphore()
    for step in range(1, rows):
        pl.semaphore_signal(
            barrier, inc=1, device_id={"row": lax.rem(z + step, rows)}, device_id_type=MESH
        )
    pl.semaphore_signal(barrier, inc=1, device_id={"col": far}, device_id_type=MESH)
    pl.semaphore_signal(barrier, inc=1, device_id={"col": mate}, device_id_type=MESH)
    pl.semaphore_signal(barrier, inc=1, device_id={"gz": other}, device_id_type=MESH)
    pl.semaphore_wait(barrier, rows + 2)

    def remote(src, dst, send, recv, where):
        return pltpu.make_async_remote_copy(
            src_ref=src, dst_ref=dst, send_sem=send, recv_sem=recv,
            device_id=where, device_id_type=MESH,
        )

    across = [
        remote(l_ref.at[v], crossed.at[v], x_send.at[v], x_recv.at[v], {"col": far})
        for v in range(levels)
    ]

    def place(v, half):
        k = c if half == 0 else far
        block = l_ref.at[v] if half == 0 else crossed.at[v]
        copy = remote(block, l_all.at[v, z], l_send.at[v, half], l_recv.at[v, z], {"row": k})
        local = pltpu.make_async_copy(block, l_all.at[v, z], loc_sem.at[v])
        return k, copy, local

    def start_place(v, half):
        k, copy, local = place(v, half)

        @pl.when(k != z)
        def _():
            copy.start()

        @pl.when(k == z)
        def _():
            local.start()

    first.wait()
    for v in range(levels):
        across[v].start()
    start_place(0, 0)

    own_live = pltpu.make_async_copy(live_ref, live_all.at[z], m_loc)
    own_live.start()
    live_out = []
    for step in range(1, rows):
        to = lax.rem(z + step, rows)
        live_out.append(
            remote(live_ref, live_all.at[z], m_send.at[step], m_recv.at[z], {"row": to})
        )
        live_out[-1].start()
    rm_copy = remote(rm_ref, rm_in, rm_send, rm_recv, {"gz": other})
    rm_copy.start()

    across[0].wait_recv()
    start_place(0, 1)
    for v in range(1, levels):
        start_place(v, 0)
        across[v].wait_recv()
        start_place(v, 1)

    own_live.wait()
    for step in range(1, rows):
        src = lax.rem(z + step, rows)
        remote(live_ref, live_all.at[src], m_send.at[step], m_recv.at[src], {"row": src}).wait_recv()

    low = 1 - z // (rows // 2)

    def order(i):
        near = jnp.int32(i) if isinstance(i, int) else i
        wrap = near // (rows // 2)
        up = rows - 1 - near + wrap * (2 * near - rows - rows // 2 + 1)
        return low * up + (1 - low) * (rows - 1 - up)

    def hop(v, a, side, to):
        return remote(
            part.at[v, a], p_in.at[v, side, a], p_send.at[v, a], p_recv.at[v, side, a], {"row": to}
        )

    right, left = lax.rem(z + 1, rows), lax.rem(z + rows - 1, rows)

    def send(v, a, side, to):
        for l in range(layers):
            part[v, a, l] = own[v, a, l].astype(jnp.bfloat16)
        hop(v, a, side, to).start()

    def item(v, a):
        relay = remote(
            l_all.at[v, a], l_all.at[v, a], relay_send.at[v, a], l_recv.at[v, a], {"col": mate}
        )

        @pl.when(gate)
        def _():
            @pl.when(a == z)
            def _():
                pltpu.make_async_copy(l_ref.at[v], l_all.at[v, z], loc_sem.at[v]).wait()

            @pl.when(a != z)
            def _():
                relay.wait_recv()

            relay.start()

        @pl.when(jnp.logical_not(gate))
        def _():
            relay.wait_recv()

        block = l_all[v, a]
        for j in range(CB):
            t = jnp.dot(
                block, u_ref[v, :, j * width : (j + 1) * width], preferred_element_type=jnp.float32
            )
            to_layer = cm_ref[v : v + 1, j : j + 1]
            live = live_all[a, v : v + 1, j : j + 1]
            for l in range(layers):
                m = jnp.where(to_layer == l, live, 0).astype(jnp.float32)
                if j == 0:
                    own[v, a, l] = t * m
                else:
                    own[v, a, l] += t * m

        @pl.when(jnp.logical_and(a > z, z == 0))
        def _():
            send(v, a, 0, right)

        @pl.when(jnp.logical_and(a < z, z == rows - 1))
        def _():
            send(v, a, 1, left)

    def collect(v, a, side):
        hop(v, a, side, right).wait_recv()
        for l in range(layers):
            own[v, a, l] += p_in[v, side, a, l].astype(jnp.float32)

    def forward(v, a):
        @pl.when(jnp.logical_and(a > z, z > 0))
        def _():
            collect(v, a, 0)
            send(v, a, 0, right)

        @pl.when(jnp.logical_and(a < z, z < rows - 1))
        def _():
            collect(v, a, 1)
            send(v, a, 1, left)

    def over_rows(step, v):
        def body(i, carry):
            step(v, order(i))
            return carry

        lax.fori_loop(0, rows, body, 0)

    for v in range(levels):
        loads[v].wait()
        over_rows(item, v)

    ways = []
    for v in range(levels):
        over_rows(forward, v)

        @pl.when(z > 0)
        def _():
            collect(v, z, 0)

        @pl.when(z < rows - 1)
        def _():
            collect(v, z, 1)

        y_out[v] = own[v, z, other].astype(jnp.bfloat16)
        way = remote(y_out.at[v], y_in.at[v], y_send.at[v], y_recv.at[v], {"gz": other})
        way.start()
        ways.append(way)

    loads[levels].wait()
    rm_copy.wait()
    for v in range(levels):
        mine = own[v, z, g].astype(jnp.bfloat16).astype(jnp.float32)
        ways[v].wait_recv()
        theirs = y_in[v].astype(jnp.float32)
        for f in range(FRB):
            lines = slice(f * width, (f + 1) * width)
            here = (rm_ref[v : v + 1, :] == f).astype(jnp.float32)
            away = (rm_in[v : v + 1, :] == f).astype(jnp.float32)
            total = here * mine + away * theirs
            out_ref[v, lines, :] = (front_ref[v, lines, :].astype(jnp.float32) - total).astype(
                out_ref.dtype
            )

    for copy in live_out:
        copy.wait_send()
    for v in range(levels):
        across[v].wait_send()
        ways[v].wait_send()
        for half in range(2):
            k, copy, _local = place(v, half)
            pl.when(k != z)(copy.wait_send)
        for a in range(rows):
            relay = remote(
                l_all.at[v, a], l_all.at[v, a], relay_send.at[v, a], l_recv.at[v, a], {"col": mate}
            )
            pl.when(gate)(relay.wait_send)
            sent = remote(
                part.at[v, a], p_in.at[v, 0, a], p_send.at[v, a], p_recv.at[v, 0, a], {"gz": other}
            )
            pl.when(a != z)(sent.wait_send)


def stationary(rows, cols, layers, lpanel, upanel, rowmap, colmap, blockmask, front_blocks):
    levels, _, width, depth = lpanel.shape
    bf16 = jnp.bfloat16
    vmem = pl.BlockSpec(memory_space=pltpu.VMEM)
    hbm = pl.BlockSpec(memory_space=pl.ANY)
    dma = pltpu.SemaphoreType.DMA
    return pl.pallas_call(
        functools.partial(kernel, rows, cols, layers, levels, width),
        out_shape=jax.ShapeDtypeStruct(front_blocks.shape, front_blocks.dtype),
        in_specs=[hbm, hbm, vmem, vmem, vmem, hbm],
        out_specs=vmem,
        scratch_shapes=[
            pltpu.VMEM((levels, width, depth), bf16),
            pltpu.VMEM(upanel[:, 0].shape, bf16),
            pltpu.VMEM(front_blocks.shape, bf16),
            pltpu.VMEM((levels, width, depth), bf16),
            pltpu.VMEM((levels, rows, width, depth), bf16),
            pltpu.VMEM((rows, levels, CB), jnp.int32),
            pltpu.VMEM((levels, rows, layers, width, width), jnp.float32),
            pltpu.VMEM((levels, rows, layers, width, width), bf16),
            pltpu.VMEM((levels, 2, rows, layers, width, width), bf16),
            pltpu.VMEM((levels, width, width), bf16),
            pltpu.VMEM((levels, width, width), bf16),
            pltpu.VMEM((levels, 1), jnp.int32),
            dma((levels + 2,)),
            dma((levels,)),
            dma((levels,)),
            dma((levels, 2)),
            dma((levels, rows)),
            dma((levels,)),
            dma((levels, rows)),
            dma((rows,)),
            dma((rows,)),
            dma,
            dma((levels, rows)),
            dma((levels, 2, rows)),
            dma((levels,)),
            dma((levels,)),
            dma,
            dma,
        ],
        compiler_params=pltpu.CompilerParams(collective_id=0, has_side_effects=True),
    )(
        lpanel[:, 0], upanel[:, 0], colmap[:, 0], blockmask[:, 0, 0], rowmap[:, 0], front_blocks
    )


def solution(mesh):
    rows, cols, layers = mesh.shape["row"], mesh.shape["col"], mesh.shape["gz"]
    body = general
    if rows == cols == 2 * layers and layers == 2:
        body = functools.partial(stationary, rows, cols, layers)
    return jax.shard_map(
        body,
        mesh=mesh,
        in_specs=(
            P(None, "gz", "row", "col"),
            P(None, "gz", "row", "col"),
            P(None, "gz", "row"),
            P(None, "gz", "col"),
            P(None, "gz", "row", "col"),
            P(None, "row", ("gz", "col")),
        ),
        out_specs=P(None, "row", ("gz", "col")),
        check_vma=False,
    )
```

```python
import functools

import jax
import jax.numpy as jnp
from jax import lax
from jax.experimental import pallas as pl
from jax.experimental.pallas import tpu as pltpu
from jax.sharding import PartitionSpec as P

CB = 4
FRB = 2
MESH = pl.DeviceIdType.MESH


def column_sums(schur, cols_of, live, layers):
    width = schur.shape[0]
    blocks = schur.reshape(width, CB, width)
    targets = cols_of[:, None] == jnp.arange(layers, dtype=jnp.int32)[None, :]
    col_select = targets.astype(jnp.float32) * live.astype(jnp.float32)[:, None]
    return jnp.einsum("bjk,jl->lbk", blocks, col_select, precision=lax.Precision.HIGHEST)


def general(lpanel, upanel, rowmap, colmap, blockmask, front_blocks):
    layers = lax.axis_size("gz")
    width = lpanel.shape[2]
    levels = lpanel.shape[0]
    tiles = []
    for depth in range(levels):
        left_rows = lax.all_gather(lpanel[depth, 0], "col", axis=1, tiled=True)
        tiles.append(
            jnp.dot(
                left_rows,
                lax.all_gather(upanel[depth, 0], "row", axis=0, tiled=True),
                preferred_element_type=jnp.float32,
            )
        )
    results = []
    every_row = lax.all_gather(rowmap[:, :, 0], "gz", axis=1, tiled=True)
    for depth in range(levels):
        sums = column_sums(tiles[depth], colmap[depth, 0], blockmask[depth, 0, 0], layers).astype(
            jnp.bfloat16
        )
        arrived = lax.all_to_all(sums, "gz", split_axis=0, concat_axis=0, tiled=True)
        row_select = (
            every_row[depth][:, None] == jnp.arange(FRB, dtype=jnp.int32)[None, :]
        ).astype(jnp.float32)
        placed = jnp.einsum(
            "sf,sbk->fbk", row_select, arrived.astype(jnp.float32), precision=lax.Precision.HIGHEST
        )
        placed = placed.reshape(FRB * width, width)
        results.append((front_blocks[depth].astype(jnp.float32) - placed).astype(jnp.bfloat16))
    return jnp.stack(results)


def kernel(
    rows, cols, layers, levels, width,
    l_hbm, u_hbm, cm_ref, live_ref, rm_ref, front_hbm, out_ref,
    l_ref, u_ref, front_ref, crossed, l_all, live_all, own, part, p_in, y_out, y_in, rm_in,
    in_sem, x_send, x_recv, l_send, l_recv, loc_sem, post_send, relay_send, m_send, m_recv, m_loc,
    p_send, p_recv, y_send, y_recv, rm_send, rm_recv,
):
    z = lax.axis_index("row")
    c = lax.axis_index("col")
    g = lax.axis_index("gz")
    far = lax.rem(c + cols // 2, cols)
    mate = c + 1 - 2 * lax.rem(c, 2)
    other = 1 - g
    gate = lax.rem(c, 2) == lax.rem(z, 2)

    loads = [pltpu.make_async_copy(u_hbm.at[v], u_ref.at[v], in_sem.at[v]) for v in range(levels)]
    loads.append(pltpu.make_async_copy(front_hbm, front_ref, in_sem.at[levels]))
    first = pltpu.make_async_copy(l_hbm, l_ref, in_sem.at[levels + 1])
    first.start()
    for load in loads:
        load.start()

    barrier = pltpu.get_barrier_semaphore()
    for step in range(1, rows):
        pl.semaphore_signal(
            barrier, inc=1, device_id={"row": lax.rem(z + step, rows)}, device_id_type=MESH
        )
    pl.semaphore_signal(barrier, inc=1, device_id={"col": far}, device_id_type=MESH)
    pl.semaphore_signal(barrier, inc=1, device_id={"col": mate}, device_id_type=MESH)
    pl.semaphore_signal(barrier, inc=1, device_id={"gz": other}, device_id_type=MESH)
    pl.semaphore_wait(barrier, rows + 2)

    def remote(src, dst, send, recv, where):
        return pltpu.make_async_remote_copy(
            src_ref=src, dst_ref=dst, send_sem=send, recv_sem=recv,
            device_id=where, device_id_type=MESH,
        )

    half = width // 2
    pieces = [slice(h * half, (h + 1) * half) for h in range(2)]

    across = [
        remote(l_ref.at[v, pieces[1]], crossed.at[v], x_send.at[v], x_recv.at[v], {"col": far})
        for v in range(levels)
    ]

    def place(v, h):
        to = c if h == 0 else far
        block = l_ref.at[v, pieces[0]] if h == 0 else crossed.at[v]
        spot = l_all.at[v, z, pieces[h]]
        copy = remote(block, spot, l_send.at[v, h], l_recv.at[v, h, z], {"row": to})
        return to, copy, block, spot

    def start_place(v, h):
        to, copy, block, spot = place(v, h)

        @pl.when(to != z)
        def _():
            copy.start()

        @pl.when(to == z)
        def _():
            pltpu.make_async_copy(block, spot, loc_sem.at[v, h]).start()

    first.wait()
    for v in range(levels):
        across[v].start()
    for v in range(levels):
        start_place(v, 0)

    own_live = pltpu.make_async_copy(live_ref, live_all.at[z], m_loc)
    own_live.start()
    live_out = []
    for step in range(1, rows):
        to = lax.rem(z + step, rows)
        live_out.append(
            remote(live_ref, live_all.at[z], m_send.at[step], m_recv.at[z], {"row": to})
        )
        live_out[-1].start()
    rm_copy = remote(rm_ref, rm_in, rm_send, rm_recv, {"gz": other})
    rm_copy.start()

    across[0].wait_recv()
    start_place(0, 1)

    own_live.wait()
    for step in range(1, rows):
        src = lax.rem(z + step, rows)
        remote(live_ref, live_all.at[src], m_send.at[step], m_recv.at[src], {"row": src}).wait_recv()

    low = 1 - z // (rows // 2)

    def order(i):
        near = jnp.int32(i) if isinstance(i, int) else i
        wrap = near // (rows // 2)
        up = rows - 1 - near + wrap * (2 * near - rows - rows // 2 + 1)
        return low * up + (1 - low) * (rows - 1 - up)

    def hop(v, a, l, side, to):
        return remote(
            part.at[v, a, l], p_in.at[v, side, a, l],
            p_send.at[v, a, l], p_recv.at[v, side, a, l], {"row": to},
        )

    turns = (other, g)
    right, left = lax.rem(z + 1, rows), lax.rem(z + rows - 1, rows)

    def send(v, a, l, side, to):
        part[v, a, l] = own[v, a, l].astype(jnp.bfloat16)
        hop(v, a, l, side, to).start()

    def passes(v, a, h):
        spot = l_all.at[v, a, pieces[h]]
        post = remote(spot, spot, post_send.at[v, a], l_recv.at[v, h, a], {"col": far})
        relay = remote(spot, spot, relay_send.at[v, h, a], l_recv.at[v, h, a], {"col": mate})
        return post, relay

    def stage(v, a):
        def gather(h):
            post, relay = passes(v, a, h)

            @pl.when(a == z)
            def _():
                spot = l_all.at[v, z, pieces[h]]
                pltpu.make_async_copy(l_ref.at[v, pieces[h]], spot, loc_sem.at[v, h]).wait()

            @pl.when(a != z)
            def _():
                relay.wait_recv()

            post.start()
            relay.start()

        def take(h):
            _post, relay = passes(v, a, h)
            relay.wait_recv()
            relay.start()

        @pl.when(c == z)
        def _():
            gather(0)
            take(1)

        @pl.when(far == z)
        def _():
            gather(1)
            take(0)

        @pl.when(jnp.logical_not(gate))
        def _():
            for h in range(2):
                passes(v, a, h)[1].wait_recv()

    def item(v, i):
        a = order(i)
        stage(v, a)
        if v + 1 < levels:
            @pl.when(i == 0)
            def _():
                across[v + 1].wait_recv()
                start_place(v + 1, 1)

        block = l_all[v, a]
        for j in range(CB):
            t = jnp.dot(
                block, u_ref[v, :, j * width : (j + 1) * width], preferred_element_type=jnp.float32
            )
            to_layer = cm_ref[v : v + 1, j : j + 1]
            live = live_all[a, v : v + 1, j : j + 1]
            for l in range(layers):
                m = jnp.where(to_layer == l, live, 0).astype(jnp.float32)
                if j == 0:
                    own[v, a, l] = t * m
                else:
                    own[v, a, l] += t * m

        @pl.when(jnp.logical_and(a > z, z == 0))
        def _():
            for l in turns:
                send(v, a, l, 0, right)

        @pl.when(jnp.logical_and(a < z, z == rows - 1))
        def _():
            for l in turns:
                send(v, a, l, 1, left)

    def collect(v, a, l, side):
        hop(v, a, l, side, right).wait_recv()
        own[v, a, l] += p_in[v, side, a, l].astype(jnp.float32)

    def forward(v, i):
        a = order(i)

        @pl.when(jnp.logical_and(a > z, z > 0))
        def _():
            for l in turns:
                collect(v, a, l, 0)
                send(v, a, l, 0, right)

        @pl.when(jnp.logical_and(a < z, z < rows - 1))
        def _():
            for l in turns:
                collect(v, a, l, 1)
                send(v, a, l, 1, left)

    def finish(v, l):
        @pl.when(z > 0)
        def _():
            collect(v, z, l, 0)

        @pl.when(z < rows - 1)
        def _():
            collect(v, z, l, 1)

    def over_rows(step, v):
        def body(i, carry):
            step(v, i)
            return carry

        lax.fori_loop(0, rows, body, 0)

    for v in range(levels):
        loads[v].wait()
        over_rows(item, v)

    ways = []
    for v in range(levels):
        over_rows(forward, v)

        finish(v, other)
        y_out[v] = own[v, z, other].astype(jnp.bfloat16)
        way = remote(y_out.at[v], y_in.at[v], y_send.at[v], y_recv.at[v], {"gz": other})
        way.start()
        ways.append(way)
        finish(v, g)

    loads[levels].wait()
    rm_copy.wait()
    for v in range(levels):
        mine = own[v, z, g].astype(jnp.bfloat16).astype(jnp.float32)
        ways[v].wait_recv()
        theirs = y_in[v].astype(jnp.float32)
        for f in range(FRB):
            lines = slice(f * width, (f + 1) * width)
            here = (rm_ref[v : v + 1, :] == f).astype(jnp.float32)
            away = (rm_in[v : v + 1, :] == f).astype(jnp.float32)
            total = here * mine + away * theirs
            out_ref[v, lines, :] = (front_ref[v, lines, :].astype(jnp.float32) - total).astype(
                out_ref.dtype
            )

    for copy in live_out:
        copy.wait_send()
    for v in range(levels):
        across[v].wait_send()
        ways[v].wait_send()
        for h in range(2):
            to, copy, _block, _spot = place(v, h)
            pl.when(to != z)(copy.wait_send)
        for a in range(rows):
            for h in range(2):
                post, relay = passes(v, a, h)
                pl.when(gate)(relay.wait_send)
                if h == 0:
                    pl.when(gate)(post.wait_send)
            for l in range(layers):
                pl.when(a != z)(hop(v, a, l, 0, right).wait_send)


def stationary(rows, cols, layers, lpanel, upanel, rowmap, colmap, blockmask, front_blocks):
    levels, _, width, depth = lpanel.shape
    bf16 = jnp.bfloat16
    vmem = pl.BlockSpec(memory_space=pltpu.VMEM)
    hbm = pl.BlockSpec(memory_space=pl.ANY)
    dma = pltpu.SemaphoreType.DMA
    return pl.pallas_call(
        functools.partial(kernel, rows, cols, layers, levels, width),
        out_shape=jax.ShapeDtypeStruct(front_blocks.shape, front_blocks.dtype),
        in_specs=[hbm, hbm, vmem, vmem, vmem, hbm],
        out_specs=vmem,
        scratch_shapes=[
            pltpu.VMEM((levels, width, depth), bf16),
            pltpu.VMEM(upanel[:, 0].shape, bf16),
            pltpu.VMEM(front_blocks.shape, bf16),
            pltpu.VMEM((levels, width // 2, depth), bf16),
            pltpu.VMEM((levels, rows, width, depth), bf16),
            pltpu.VMEM((rows, levels, CB), jnp.int32),
            pltpu.VMEM((levels, rows, layers, width, width), jnp.float32),
            pltpu.VMEM((levels, rows, layers, width, width), bf16),
            pltpu.VMEM((levels, 2, rows, layers, width, width), bf16),
            pltpu.VMEM((levels, width, width), bf16),
            pltpu.VMEM((levels, width, width), bf16),
            pltpu.VMEM((levels, 1), jnp.int32),
            dma((levels + 2,)),
            dma((levels,)),
            dma((levels,)),
            dma((levels, 2)),
            dma((levels, 2, rows)),
            dma((levels, 2)),
            dma((levels, rows)),
            dma((levels, 2, rows)),
            dma((rows,)),
            dma((rows,)),
            dma,
            dma((levels, rows, layers)),
            dma((levels, 2, rows, layers)),
            dma((levels,)),
            dma((levels,)),
            dma,
            dma,
        ],
        compiler_params=pltpu.CompilerParams(collective_id=0, has_side_effects=True),
    )(
        lpanel[:, 0], upanel[:, 0], colmap[:, 0], blockmask[:, 0, 0], rowmap[:, 0], front_blocks
    )


def solution(mesh):
    rows, cols, layers = mesh.shape["row"], mesh.shape["col"], mesh.shape["gz"]
    body = general
    if rows == cols == 2 * layers and layers == 2:
        body = functools.partial(stationary, rows, cols, layers)
    return jax.shard_map(
        body,
        mesh=mesh,
        in_specs=(
            P(None, "gz", "row", "col"),
            P(None, "gz", "row", "col"),
            P(None, "gz", "row"),
            P(None, "gz", "col"),
            P(None, "gz", "row", "col"),
            P(None, "row", ("gz", "col")),
        ),
        out_specs=P(None, "row", ("gz", "col")),
        check_vma=False,
    )
```

```python
import functools

import jax
import jax.numpy as jnp
from jax import lax
from jax.experimental import pallas as pl
from jax.experimental.pallas import tpu as pltpu
from jax.sharding import PartitionSpec as P

CB = 4
FRB = 2
MESH = pl.DeviceIdType.MESH


def column_sums(schur, cols_of, live, layers):
    width = schur.shape[0]
    blocks = schur.reshape(width, CB, width)
    targets = cols_of[:, None] == jnp.arange(layers, dtype=jnp.int32)[None, :]
    col_select = targets.astype(jnp.float32) * live.astype(jnp.float32)[:, None]
    return jnp.einsum("bjk,jl->lbk", blocks, col_select, precision=lax.Precision.HIGHEST)


def general(lpanel, upanel, rowmap, colmap, blockmask, front_blocks):
    layers = lax.axis_size("gz")
    width = lpanel.shape[2]
    levels = lpanel.shape[0]
    tiles = []
    for depth in range(levels):
        left_rows = lax.all_gather(lpanel[depth, 0], "col", axis=1, tiled=True)
        tiles.append(
            jnp.dot(
                left_rows,
                lax.all_gather(upanel[depth, 0], "row", axis=0, tiled=True),
                preferred_element_type=jnp.float32,
            )
        )
    results = []
    every_row = lax.all_gather(rowmap[:, :, 0], "gz", axis=1, tiled=True)
    for depth in range(levels):
        sums = column_sums(tiles[depth], colmap[depth, 0], blockmask[depth, 0, 0], layers).astype(
            jnp.bfloat16
        )
        arrived = lax.all_to_all(sums, "gz", split_axis=0, concat_axis=0, tiled=True)
        row_select = (
            every_row[depth][:, None] == jnp.arange(FRB, dtype=jnp.int32)[None, :]
        ).astype(jnp.float32)
        placed = jnp.einsum(
            "sf,sbk->fbk", row_select, arrived.astype(jnp.float32), precision=lax.Precision.HIGHEST
        )
        placed = placed.reshape(FRB * width, width)
        results.append((front_blocks[depth].astype(jnp.float32) - placed).astype(jnp.bfloat16))
    return jnp.stack(results)


def kernel(
    rows, cols, layers, levels, width,
    l_hbm, u_hbm, cm_ref, live_ref, rm_ref, front_hbm, out_ref,
    l_ref, u_ref, front_ref, crossed, l_all, live_all, own, part, p_in, y_out, y_in, rm_in,
    in_sem, x_send, x_recv, l_send, l_recv, loc_sem, post_send, relay_send, m_send, m_recv, m_loc,
    p_send, p_recv, y_send, y_recv, rm_send, rm_recv,
):
    z = lax.axis_index("row")
    c = lax.axis_index("col")
    g = lax.axis_index("gz")
    far = lax.rem(c + cols // 2, cols)
    mate = c + 1 - 2 * lax.rem(c, 2)
    other = 1 - g
    gate = lax.rem(c, 2) == lax.rem(z, 2)

    loads = [pltpu.make_async_copy(u_hbm.at[v], u_ref.at[v], in_sem.at[v]) for v in range(levels)]
    loads.append(pltpu.make_async_copy(front_hbm, front_ref, in_sem.at[levels]))
    first = pltpu.make_async_copy(l_hbm, l_ref, in_sem.at[levels + 1])
    first.start()
    for load in loads:
        load.start()

    barrier = pltpu.get_barrier_semaphore()
    for step in range(1, rows):
        pl.semaphore_signal(
            barrier, inc=1, device_id={"row": lax.rem(z + step, rows)}, device_id_type=MESH
        )
    pl.semaphore_signal(barrier, inc=1, device_id={"col": far}, device_id_type=MESH)
    pl.semaphore_signal(barrier, inc=1, device_id={"col": mate}, device_id_type=MESH)
    pl.semaphore_signal(barrier, inc=1, device_id={"gz": other}, device_id_type=MESH)
    pl.semaphore_wait(barrier, rows + 2)

    def remote(src, dst, send, recv, where):
        return pltpu.make_async_remote_copy(
            src_ref=src, dst_ref=dst, send_sem=send, recv_sem=recv,
            device_id=where, device_id_type=MESH,
        )

    half = width // 2
    pieces = [slice(h * half, (h + 1) * half) for h in range(2)]

    across = [
        remote(l_ref.at[v, pieces[1]], crossed.at[v], x_send.at[v], x_recv.at[v], {"col": far})
        for v in range(levels)
    ]

    def place(v, h):
        to = c if h == 0 else far
        block = l_ref.at[v, pieces[0]] if h == 0 else crossed.at[v]
        spot = l_all.at[v, z, pieces[h]]
        copy = remote(block, spot, l_send.at[v, h], l_recv.at[v, h, z], {"row": to})
        return to, copy, block, spot

    def start_place(v, h):
        to, copy, block, spot = place(v, h)

        @pl.when(to != z)
        def _():
            copy.start()

        @pl.when(to == z)
        def _():
            pltpu.make_async_copy(block, spot, loc_sem.at[v, h]).start()

    first.wait()
    for v in range(levels):
        across[v].start()
    for v in range(levels):
        start_place(v, 0)

    own_live = pltpu.make_async_copy(live_ref, live_all.at[z], m_loc)
    own_live.start()
    live_out = []
    for step in range(1, rows):
        to = lax.rem(z + step, rows)
        live_out.append(
            remote(live_ref, live_all.at[z], m_send.at[step], m_recv.at[z], {"row": to})
        )
        live_out[-1].start()
    rm_copy = remote(rm_ref, rm_in, rm_send, rm_recv, {"gz": other})
    rm_copy.start()

    across[0].wait_recv()
    start_place(0, 1)

    own_live.wait()
    for step in range(1, rows):
        src = lax.rem(z + step, rows)
        remote(live_ref, live_all.at[src], m_send.at[step], m_recv.at[src], {"row": src}).wait_recv()

    low = 1 - z // (rows // 2)

    def order(i):
        near = jnp.int32(i) if isinstance(i, int) else i
        wrap = near // (rows // 2)
        up = rows - 1 - near + wrap * (2 * near - rows - rows // 2 + 1)
        return low * up + (1 - low) * (rows - 1 - up)

    def hop(v, a, l, side, to):
        return remote(
            part.at[v, a, l], p_in.at[v, side, a, l],
            p_send.at[v, a, l], p_recv.at[v, side, a, l], {"row": to},
        )

    turns = (other, g)
    right, left = lax.rem(z + 1, rows), lax.rem(z + rows - 1, rows)

    def send(v, a, l, side, to):
        part[v, a, l] = own[v, a, l].astype(jnp.bfloat16)
        hop(v, a, l, side, to).start()

    def passes(v, a, h):
        spot = l_all.at[v, a, pieces[h]]
        post = remote(spot, spot, post_send.at[v, a], l_recv.at[v, h, a], {"col": far})
        relay = remote(spot, spot, relay_send.at[v, h, a], l_recv.at[v, h, a], {"col": mate})
        return post, relay

    def gather_half(v, a, h):
        post, relay = passes(v, a, h)

        @pl.when(a == z)
        def _():
            spot = l_all.at[v, z, pieces[h]]
            pltpu.make_async_copy(l_ref.at[v, pieces[h]], spot, loc_sem.at[v, h]).wait()

        @pl.when(a != z)
        def _():
            relay.wait_recv()

        post.start()
        relay.start()

    def take_half(v, a, h):
        _post, relay = passes(v, a, h)
        relay.wait_recv()
        relay.start()

    def gather(v, i):
        a = order(i)
        pl.when(c == z)(lambda: gather_half(v, a, 0))
        pl.when(far == z)(lambda: gather_half(v, a, 1))

    def take(v, i):
        a = order(i)
        pl.when(c == z)(lambda: take_half(v, a, 1))
        pl.when(far == z)(lambda: take_half(v, a, 0))

    def item(v, i):
        a = order(i)

        @pl.when(i == 0)
        def _():
            take(v, i)

        @pl.when(i < rows - 1)
        def _():
            take(v, i + 1)

        @pl.when(jnp.logical_not(gate))
        def _():
            for h in range(2):
                passes(v, a, h)[1].wait_recv()

        block = l_all[v, a]
        for j in range(CB):
            t = jnp.dot(
                block, u_ref[v, :, j * width : (j + 1) * width], preferred_element_type=jnp.float32
            )
            to_layer = cm_ref[v : v + 1, j : j + 1]
            live = live_all[a, v : v + 1, j : j + 1]
            for l in range(layers):
                m = jnp.where(to_layer == l, live, 0).astype(jnp.float32)
                if j == 0:
                    own[v, a, l] = t * m
                else:
                    own[v, a, l] += t * m

        @pl.when(jnp.logical_and(a > z, z == 0))
        def _():
            for l in turns:
                send(v, a, l, 0, right)

        @pl.when(jnp.logical_and(a < z, z == rows - 1))
        def _():
            for l in turns:
                send(v, a, l, 1, left)

        if v + 1 < levels:
            gather(v + 1, i)

    def collect(v, a, l, side):
        hop(v, a, l, side, right).wait_recv()
        own[v, a, l] += p_in[v, side, a, l].astype(jnp.float32)

    def forward(v, i):
        a = order(i)

        @pl.when(jnp.logical_and(a > z, z > 0))
        def _():
            for l in turns:
                collect(v, a, l, 0)
                send(v, a, l, 0, right)

        @pl.when(jnp.logical_and(a < z, z < rows - 1))
        def _():
            for l in turns:
                collect(v, a, l, 1)
                send(v, a, l, 1, left)

    def finish(v, l):
        @pl.when(z > 0)
        def _():
            collect(v, z, l, 0)

        @pl.when(z < rows - 1)
        def _():
            collect(v, z, l, 1)

    def over_rows(step, v):
        def body(i, carry):
            step(v, i)
            return carry

        lax.fori_loop(0, rows, body, 0)

    for v in range(levels):
        if v == 0:
            over_rows(gather, v)
        if v + 1 < levels:
            across[v + 1].wait_recv()
            start_place(v + 1, 1)
        loads[v].wait()
        over_rows(item, v)

    ways = []
    for v in range(levels):
        over_rows(forward, v)

        finish(v, other)
        y_out[v] = own[v, z, other].astype(jnp.bfloat16)
        way = remote(y_out.at[v], y_in.at[v], y_send.at[v], y_recv.at[v], {"gz": other})
        way.start()
        ways.append(way)
        finish(v, g)

    loads[levels].wait()
    rm_copy.wait()
    for v in range(levels):
        mine = own[v, z, g].astype(jnp.bfloat16).astype(jnp.float32)
        ways[v].wait_recv()
        theirs = y_in[v].astype(jnp.float32)
        for f in range(FRB):
            lines = slice(f * width, (f + 1) * width)
            here = (rm_ref[v : v + 1, :] == f).astype(jnp.float32)
            away = (rm_in[v : v + 1, :] == f).astype(jnp.float32)
            total = here * mine + away * theirs
            out_ref[v, lines, :] = (front_ref[v, lines, :].astype(jnp.float32) - total).astype(
                out_ref.dtype
            )

    for copy in live_out:
        copy.wait_send()
    for v in range(levels):
        across[v].wait_send()
        ways[v].wait_send()
        for h in range(2):
            to, copy, _block, _spot = place(v, h)
            pl.when(to != z)(copy.wait_send)
        for a in range(rows):
            for h in range(2):
                post, relay = passes(v, a, h)
                pl.when(gate)(relay.wait_send)
                if h == 0:
                    pl.when(gate)(post.wait_send)
            for l in range(layers):
                pl.when(a != z)(hop(v, a, l, 0, right).wait_send)


def stationary(rows, cols, layers, lpanel, upanel, rowmap, colmap, blockmask, front_blocks):
    levels, _, width, depth = lpanel.shape
    bf16 = jnp.bfloat16
    vmem = pl.BlockSpec(memory_space=pltpu.VMEM)
    hbm = pl.BlockSpec(memory_space=pl.ANY)
    dma = pltpu.SemaphoreType.DMA
    return pl.pallas_call(
        functools.partial(kernel, rows, cols, layers, levels, width),
        out_shape=jax.ShapeDtypeStruct(front_blocks.shape, front_blocks.dtype),
        in_specs=[hbm, hbm, vmem, vmem, vmem, hbm],
        out_specs=vmem,
        scratch_shapes=[
            pltpu.VMEM((levels, width, depth), bf16),
            pltpu.VMEM(upanel[:, 0].shape, bf16),
            pltpu.VMEM(front_blocks.shape, bf16),
            pltpu.VMEM((levels, width // 2, depth), bf16),
            pltpu.VMEM((levels, rows, width, depth), bf16),
            pltpu.VMEM((rows, levels, CB), jnp.int32),
            pltpu.VMEM((levels, rows, layers, width, width), jnp.float32),
            pltpu.VMEM((levels, rows, layers, width, width), bf16),
            pltpu.VMEM((levels, 2, rows, layers, width, width), bf16),
            pltpu.VMEM((levels, width, width), bf16),
            pltpu.VMEM((levels, width, width), bf16),
            pltpu.VMEM((levels, 1), jnp.int32),
            dma((levels + 2,)),
            dma((levels,)),
            dma((levels,)),
            dma((levels, 2)),
            dma((levels, 2, rows)),
            dma((levels, 2)),
            dma((levels, rows)),
            dma((levels, 2, rows)),
            dma((rows,)),
            dma((rows,)),
            dma,
            dma((levels, rows, layers)),
            dma((levels, 2, rows, layers)),
            dma((levels,)),
            dma((levels,)),
            dma,
            dma,
        ],
        compiler_params=pltpu.CompilerParams(collective_id=0, has_side_effects=True),
    )(
        lpanel[:, 0], upanel[:, 0], colmap[:, 0], blockmask[:, 0, 0], rowmap[:, 0], front_blocks
    )


def solution(mesh):
    rows, cols, layers = mesh.shape["row"], mesh.shape["col"], mesh.shape["gz"]
    body = general
    if rows == cols == 2 * layers and layers == 2:
        body = functools.partial(stationary, rows, cols, layers)
    return jax.shard_map(
        body,
        mesh=mesh,
        in_specs=(
            P(None, "gz", "row", "col"),
            P(None, "gz", "row", "col"),
            P(None, "gz", "row"),
            P(None, "gz", "col"),
            P(None, "gz", "row", "col"),
            P(None, "row", ("gz", "col")),
        ),
        out_specs=P(None, "row", ("gz", "col")),
        check_vma=False,
    )
```
